256 devices in a mesh: dp: 32 (over y, x, core), feat: 8 (over z).
Axes of the slice: x: 4, y: 4, z: 8, core: 2. Of those that a mesh axis runs over, the one named last changes fastest.
Arguments:
- hidden_states: bfloat16 [512, 256, 1152], P(('dp', 'feat')), may hold values from -6 to 6
- teacher: bfloat16 [512, 256, 1024], P('dp', None, 'feat'), may hold values from -6 to 6
- proj_in: bfloat16 [2048, 1152], replicated, may hold values from -0.1875 to 0.1875
- bias_in: float32 [2048], replicated, may hold values from -3 to 3
- proj_out: bfloat16 [2048, 1024], replicated, may hold values from -0.125 to 0.125
- bias_out: float32 [1024], replicated, may hold values from -3 to 3
Outputs:
- grad_proj_in: float32 [2048, 1152], P(('dp', 'feat'))
- grad_bias_in: float32 [2048], P(('dp', 'feat'))
- grad_proj_out: float32 [2048, 1024], P(('dp', 'feat'))
- grad_bias_out: float32 [1024], replicated
- grad_hidden: bfloat16 [512, 256, 1152], P(('dp', 'feat'))
- loss: float32 [], replicated
The draws below stay inside these ranges and needn't reach their ends.
All inputs are finite; a program needn't handle non-finite values.
Results may differ from the reference program's by a relative error of at most 0.0095.
The reference program's roundings to bfloat16 on the way (of `act`, `cot` and `dpre`) count: a program that leaves them out, or rounds other values in their place, can miss the bound.
Values may be sent and summed in bfloat16 or wider, within the bound.
No kernel may reach another device: no remote copies, remote signals or barrier semaphores. Data moves between devices by JAX's collectives and lax.ppermute only.
A program may use at most 128 MiB of HBM per device.

```python
import jax
import jax.numpy as jnp
from jax import lax

D = 1152
H = 2048
E = 1024
L = 256
B_DEV = 2
BATCH = 512
N_FEAT = 8


def levels(own_key, shape, shards, smallest, top_value):
    def one(position, shards_of):
        draws = jax.random.uniform(jax.random.fold_in(jax.random.fold_in(own_key, 6), position), (shards_of,), jnp.float32, smallest / len(shards), top_value / len(shards))
        return jnp.repeat(jnp.exp(draws), shape[position] // shards_of).reshape((-1,) + (1,) * (len(shape) - position - 1))

    level = one(*shards[0])
    for cut in shards[1:]:
        level = level * one(*cut)
    return level


def gaussian(key, extent, deviation, bound, cuts=(), dtype=jnp.bfloat16):
    result = jax.random.normal(key, extent, jnp.float32) * deviation
    if len(cuts) > 0:
        result = levels(key, extent, cuts, -0.22, 0.18) * result
    return jnp.clip(result, min=-bound, max=bound).astype(dtype)


def setup_inputs(seed: int = 0) -> dict:
    streams_of = jax.random.split(jax.random.key(seed), 7)
    hidden_states = gaussian(streams_of[0], (BATCH, L, D), 1.0, 6.0, ((0, 256),))
    teacher = gaussian(streams_of[1], (BATCH, L, E), 1.0, 6.0, ((0, 32), (2, 8)))
    proj_in = gaussian(streams_of[2], (H, D), D ** -0.5, 0.1875)
    bias_in = gaussian(streams_of[3], (H,), 0.5, 3.0, (), jnp.float32)
    proj_out = gaussian(streams_of[4], (H, E), H ** -0.5, 0.125)
    bias_out = gaussian(streams_of[5], (E,), 0.5, 3.0, (), jnp.float32)
    return {"hidden_states": hidden_states, "teacher": teacher, "proj_in": proj_in, "bias_in": bias_in, "proj_out": proj_out, "bias_out": bias_out}


epsilon = 1e-06

def reference(hidden_states, teacher, proj_in, bias_in, proj_out, bias_out):
    scale = 1.0 / float(BATCH * L)
    group = B_DEV * N_FEAT
    blocks = BATCH // group
    hid_blocks = hidden_states.reshape(blocks, group * L, D)
    tea_blocks = teacher.reshape(blocks, group * L, E)

    def step(carry, items):
        rows, target_raw = items
        g_in, b_in, g_out, b_out, loss_sum = carry
        pre = lax.dot_general(rows, proj_in, (((1,), (1,)), ((), ())), preferred_element_type=jnp.float32) + bias_in
        act = jax.nn.silu(pre).astype(jnp.bfloat16)
        out = jnp.dot(act, proj_out, preferred_element_type=jnp.float32) + bias_out
        target = target_raw.astype(jnp.float32)
        zz = lax.optimization_barrier(jnp.sum(out * out, axis=1))
        yy = lax.optimization_barrier(jnp.sum(target * target, axis=1))
        zy = lax.optimization_barrier(jnp.sum(out * target, axis=1))
        norm_z = jnp.sqrt(zz + epsilon)
        norm_y = jnp.sqrt(yy + epsilon)
        cosine = zy / (norm_z * norm_y)
        cot = (-(target / (norm_z * norm_y)[:, None] - (cosine / (norm_z * norm_z))[:, None] * out)).astype(jnp.bfloat16)
        back = lax.dot_general(cot, proj_out, (((1,), (1,)), ((), ())), preferred_element_type=jnp.float32)
        sig = jax.nn.sigmoid(pre)
        dpre = (back * sig * (1.0 + pre * (1.0 - sig))).astype(jnp.bfloat16)
        g_out = g_out + lax.dot_general(act, cot, (((0,), (0,)), ((), ())), preferred_element_type=jnp.float32)
        b_out = b_out + lax.optimization_barrier(jnp.sum(cot.astype(jnp.float32), axis=0))
        g_in = g_in + lax.dot_general(dpre, rows, (((0,), (0,)), ((), ())), preferred_element_type=jnp.float32)
        b_in = b_in + lax.optimization_barrier(jnp.sum(dpre.astype(jnp.float32), axis=0))
        loss_sum = loss_sum + jnp.sum(cosine)
        grad_rows = jnp.dot(dpre, proj_in, preferred_element_type=jnp.float32).astype(jnp.bfloat16)
        return ((g_in, b_in, g_out, b_out, loss_sum), grad_rows)
    init = (jnp.zeros((H, D), jnp.float32), jnp.zeros((H,), jnp.float32), jnp.zeros((H, E), jnp.float32), jnp.zeros((E,), jnp.float32), jnp.zeros((), jnp.float32))
    carry, grad_rows = lax.scan(step, init, (hid_blocks, tea_blocks))
    g_in, b_in, g_out, b_out, loss_sum = carry
    return (g_in * scale, b_in * scale, g_out * scale, b_out * scale, grad_rows.reshape(BATCH, L, D), -loss_sum * scale)
```

```python
import jax
import jax.numpy as jnp
from jax import lax
from jax.sharding import Mesh
from jax.sharding import PartitionSpec as P

Y, X, C, Z = "dp_0", "dp_1", "dp_2", "feat"
DP = (Y, X, C)
DP_FEAT = (Y, X, C, Z)

epsilon = 1e-06
f32, bf16 = jnp.float32, jnp.bfloat16


def shift(x, axis, k):
    n = lax.axis_size(axis)
    return lax.ppermute(x, axis, [(i, (i + k) % n) for i in range(n)])


def pick(x, index, axis):
    return lax.dynamic_index_in_dim(x, index, axis, keepdims=False)


def high_low(v):
    high = lax.reduce_precision(v, 8, 7)
    return high, v - high


def exchange(axis, make):
    me = lax.axis_index(axis)
    return {k: shift(make(lax.rem(me + k + 4, 4)), axis, k) for k in (2, 1, -1)}


def total(own, got):
    return (own + got[2]) + (got[1] + got[-1])


def on_device(hidden_states, teacher, proj_in, bias_in, proj_out, bias_out):
    samples, seq, width = hidden_states.shape
    units = proj_in.shape[0]
    channels = proj_out.shape[1]
    ny, nx, nc, nz = (lax.axis_size(a) for a in DP_FEAT)
    y, x, c, z = (lax.axis_index(a) for a in DP_FEAT)
    tokens = samples * seq
    chunk = channels // nz
    block = units // (ny * nx * nc)
    half = units // nc
    share = block // nz
    scale = 1.0 / float(tokens * ny * nx * nc * nz)

    rows = hidden_states.reshape(tokens, width)
    rows_p = shift(rows, C, 1)

    pieces = {0: lax.dynamic_slice_in_dim(teacher, z * samples, samples, 0)}
    for k in (4, 3, -3, 2, -2, 1, -1):
        to = lax.rem(z + k + nz, nz)
        pieces[k] = shift(lax.dynamic_slice_in_dim(teacher, to * samples, samples, 0), Z, k)

    def halves(w):
        w = w.reshape((ny * nx, nc, block) + w.shape[1:])
        return [pick(w, i, 1).reshape((half,) + w.shape[3:]) for i in (c, 1 - c)]

    in_mine, in_other = halves(proj_in)
    out_mine, out_other = halves(proj_out)
    bias_mine, _ = halves(bias_in)

    def nt(a, b):
        return lax.dot_general(a, b, (((1,), (1,)), ((), ())), preferred_element_type=f32)

    def tn(a, b):
        return lax.dot_general(a, b, (((0,), (0,)), ((), ())), preferred_element_type=f32)

    def nn(a, b):
        return jnp.dot(a, b, preferred_element_type=f32)

    pre, pre_p = nt(rows, in_mine) + bias_mine, nt(rows_p, in_mine) + bias_mine
    act, act_p = jax.nn.silu(pre).astype(bf16), jax.nn.silu(pre_p).astype(bf16)
    act_r = shift(act_p, C, 1)
    out = nn(act, out_mine) + nn(act_r, out_other) + bias_out

    target = jnp.zeros((tokens, channels), bf16)
    for k, piece in pieces.items():
        of = lax.rem(z - k + nz, nz)
        target = lax.dynamic_update_slice(target, piece.reshape(tokens, chunk), (0, of * chunk))
    target = target.astype(f32)
    zz = jnp.sum(out * out, axis=1)
    yy = jnp.sum(target * target, axis=1)
    zy = jnp.sum(out * target, axis=1)
    norm_z = jnp.sqrt(zz + epsilon)
    norm_y = jnp.sqrt(yy + epsilon)
    cosine = zy / (norm_z * norm_y)
    cot = (
        -(target / (norm_z * norm_y)[:, None] - (cosine / (norm_z * norm_z))[:, None] * out)
    ).astype(bf16)
    cot_p = shift(cot, C, 1)
    small = jnp.concatenate(
        [jnp.sum(cot.astype(f32), axis=0), jnp.sum(cosine)[None], jnp.zeros((511,), f32)]
    ).reshape(3, 512)
    small = small + shift(small, C, 1)

    def pack(v, rows_to, cols_to):
        both = jnp.concatenate(high_low(v), axis=0).astype(bf16)
        return jnp.pad(both, ((0, rows_to - 6), (0, cols_to - 512)))

    def unpack(r):
        r = r.astype(f32)
        return r[0:3, :512] + r[3:6, :512]

    last = tn(act, cot) + tn(act_p, cot_p)
    last = last.reshape(ny, nx, block, channels)
    cut = channels // 2
    pack_small = pack(small, 16, cut)
    got = exchange(
        X,
        lambda j: jnp.concatenate(
            [pick(last, j, 1)[:, :, :cut].astype(bf16).reshape(ny * block, cut), pack_small], axis=0
        ),
    )
    last_a = total(
        pick(last, x, 1)[:, :, :cut],
        {k: v[: ny * block].reshape(ny, block, cut).astype(f32) for k, v in got.items()},
    )
    small = total(unpack(pack_small), {k: unpack(v[ny * block :]) for k, v in got.items()})
    got = exchange(Y, lambda j: pick(last, j, 0)[:, :, cut:].astype(bf16))
    last_b = total(pick(last, y, 0)[:, :, cut:], {k: v.astype(f32) for k, v in got.items()})

    back, back_p = nt(cot, out_mine), nt(cot_p, out_mine)

    def through(back, pre):
        sig = jax.nn.sigmoid(pre)
        return (back * sig * (1.0 + pre * (1.0 - sig))).astype(bf16)

    dpre, dpre_p = through(back, pre), through(back_p, pre_p)
    dpre_r = shift(dpre_p, C, 1)
    first = tn(dpre, rows) + tn(dpre_p, rows_p)
    bias = jnp.sum(dpre.astype(f32), axis=0) + jnp.sum(dpre_p.astype(f32), axis=0)
    wide = 640
    rest = width - wide
    first = first.reshape(ny, nx, block, width)
    bias = bias.reshape(ny, nx, block, 1)

    def with_bias(g, b):
        high, low = high_low(b)
        lane = lax.broadcasted_iota(jnp.int32, b.shape[:-1] + (wide - rest,), b.ndim - 1)
        return jnp.concatenate([g, jnp.where(lane == 0, high, low)], axis=-1).astype(bf16)

    def split_bias(r):
        r = r.astype(f32)
        return r[..., :rest], r[..., rest : rest + 1] + r[..., rest + 1 : rest + 2]

    got = exchange(X, lambda j: pick(first, j, 1)[:, :, :wide].astype(bf16))
    first_a = total(pick(first, x, 1)[:, :, :wide], {k: v.astype(f32) for k, v in got.items()})
    got = exchange(Y, lambda j: with_bias(pick(first, j, 0)[:, :, wide:], pick(bias, j, 0)))
    got = {k: split_bias(v) for k, v in got.items()}
    first_b = total(pick(first, y, 0)[:, :, wide:], {k: v[0] for k, v in got.items()})
    bias = total(pick(bias, y, 0), {k: v[1] for k, v in got.items()})

    pack_small = pack(small, 16, cut + wide)
    got = exchange(
        Y,
        lambda j: jnp.concatenate(
            [
                jnp.concatenate([pick(last_a, j, 0), pick(first_a, j, 0)], axis=-1).astype(bf16),
                pack_small,
            ],
            axis=0,
        ),
    )
    sum_a = total(
        jnp.concatenate([pick(last_a, y, 0), pick(first_a, y, 0)], axis=-1),
        {k: v[:block].astype(f32) for k, v in got.items()},
    )
    small = total(unpack(pack_small), {k: unpack(v[block:]) for k, v in got.items()})
    got = exchange(
        X,
        lambda j: jnp.concatenate(
            [pick(last_b, j, 0).astype(bf16), with_bias(pick(first_b, j, 0), pick(bias, j, 0))],
            axis=-1,
        ),
    )
    sum_b = total(
        jnp.concatenate([pick(last_b, x, 0), pick(first_b, x, 0)], axis=-1),
        {k: v[:, : cut + rest].astype(f32) for k, v in got.items()},
    )
    bias = total(
        pick(bias, x, 0), {k: split_bias(v[:, cut:])[1] for k, v in got.items()}
    )

    joint = jnp.concatenate(
        [
            sum_a[:, :cut].astype(bf16),
            sum_b[:, :cut].astype(bf16),
            sum_a[:, cut:].astype(bf16),
            with_bias(sum_b[:, cut:], bias),
        ],
        axis=-1,
    ).reshape(nz, share, channels + 2 * wide)
    tail = jnp.broadcast_to(pack(small, 8, 512)[None], (nz, 8, 512))
    joint = jnp.concatenate([joint, tail], axis=-1)
    joint = lax.all_to_all(joint, Z, split_axis=0, concat_axis=0, tiled=True).astype(f32)
    joint = jnp.sum(joint, axis=0)
    small = joint[0:3, channels + 2 * wide :] + joint[3:6, channels + 2 * wide :]
    small = small.reshape(-1)
    grad_last = joint[:, :channels]
    grad_first = joint[:, channels : channels + width]
    grad_bias = joint[:, channels + width] + joint[:, channels + width + 1]

    grad_hidden = (
        (nn(dpre, in_mine) + nn(dpre_r, in_other)).astype(bf16).reshape(samples, seq, width)
    )
    return (
        grad_first * scale,
        grad_bias * scale,
        grad_last * scale,
        small[:channels] * scale,
        grad_hidden,
        -small[channels] * scale,
    )


def solution(mesh):
    finer = Mesh(mesh.devices.reshape(4, 4, 2, mesh.shape["feat"]), DP_FEAT)
    return jax.shard_map(
        on_device,
        mesh=finer,
        in_specs=(P(DP_FEAT, None, None), P(DP, None, Z), P(), P(), P(), P()),
        out_specs=(
            P(DP_FEAT, None),
            P(DP_FEAT),
            P(DP_FEAT, None),
            P(),
            P(DP_FEAT, None, None),
            P(),
        ),
        check_vma=False,
    )
```

```python
import functools

import jax
import jax.numpy as jnp
from jax import lax
from jax.experimental import pallas as pl
from jax.experimental.pallas import tpu as pltpu
from jax.sharding import Mesh
from jax.sharding import PartitionSpec as P


Y, X, C, Z = "dp_0", "dp_1", "dp_2", "feat"
DP = (Y, X, C)
DP_FEAT = (Y, X, C, Z)

epsilon = 1e-06
f32, bf16 = jnp.float32, jnp.bfloat16
RING = 4
SHIFTS = (1, 3, 2)
ROWS = 8
MIB = 1 << 20

VMEM = pl.BlockSpec(memory_space=pltpu.VMEM)
HBM = pl.BlockSpec(memory_space=pltpu.HBM)


def shift(x, axis, k):
    n = lax.axis_size(axis)
    return lax.ppermute(x, axis, [(i, (i + k) % n) for i in range(n)])


def nt(a, b):
    return lax.dot_general(a, b, (((1,), (1,)), ((), ())), preferred_element_type=f32)


def nn(a, b):
    return jnp.dot(a, b, preferred_element_type=f32)


def high_low(v):
    high = v.astype(bf16)
    return high, (v - high.astype(f32)).astype(bf16)


def total(own, got):
    at1, at3, at2 = got
    return (own + at2) + (at1 + at3)


def call(body, ins, outs, scratch=(), flops=0, limit=16):
    return pl.pallas_call(
        body,
        out_shape=[jax.ShapeDtypeStruct(s, d) for s, d in outs],
        in_specs=ins,
        out_specs=[VMEM] * len(outs),
        scratch_shapes=list(scratch),
        compiler_params=pltpu.CompilerParams(vmem_limit_bytes=limit * MIB),
        cost_estimate=pl.CostEstimate(flops=flops, bytes_accessed=4 * MIB, transcendentals=0),
    )


def gather(w_ref, to_ref, sems, core):
    y, x = lax.axis_index(Y), lax.axis_index(X)
    block = w_ref.shape[3]
    copies = []
    for kx in range(RING):
        for ky in range(RING):
            at = kx * RING + ky
            copies.append(
                pltpu.make_async_copy(
                    w_ref.at[lax.rem(y + ky, RING), lax.rem(x + kx, RING), core],
                    to_ref.at[pl.ds(at * block, block)],
                    sems.at[at],
                )
            )
    for copy in copies:
        copy.start()
    return copies


def identity(n):
    row = lax.broadcasted_iota(jnp.int32, (n, n), 0)
    return jnp.where(row == lax.broadcasted_iota(jnp.int32, (n, n), 1), 1.0, 0.0).astype(bf16)


def turn(ref, to):
    eye = identity(ref.shape[1])

    @pl.loop(0, ref.shape[0] // 256)
    def _(i):
        at = pl.ds(pl.multiple_of(i * 256, 256), 256)
        to[:, at] = nt(eye, ref[at, :]).astype(bf16)


def first_kernel(
    rows, rows_p, w_in, w_out, bias, act_t, act_pt, slope, slope_p, act, act_p, in_mine, in_other,
    out_mine, out_other, col, s0, s1, s2, s3,
):
    y, x, c = lax.axis_index(Y), lax.axis_index(X), lax.axis_index(C)
    now = gather(w_in, in_mine, s0, c)
    later = gather(w_out, out_mine, s1, c) + gather(w_out, out_other, s2, 1 - c)
    later += gather(w_in, in_other, s3, 1 - c)
    block = w_in.shape[3]
    for kx in range(RING):
        for ky in range(RING):
            of = (lax.rem(y + ky, RING) * RING + lax.rem(x + kx, RING)) * 2 + c
            col[pl.ds((kx * RING + ky) * block, block), :] = bias[
                pl.ds(pl.multiple_of(of * block, block), block), :
            ]
    for copy in now:
        copy.wait()

    for r, a, s in ((rows, act_t, slope), (rows_p, act_pt, slope_p)):

        @pl.loop(0, r.shape[0] // 256)
        def _(i):
            at = pl.ds(pl.multiple_of(i * 256, 256), 256)
            pre = nt(in_mine[...], r[at, :]) + col[...]
            sig = jax.nn.sigmoid(pre)
            a[:, at] = (pre * sig).astype(bf16)
            s[:, at] = sig * (1.0 + pre * (1.0 - sig))

    turn(act_pt, act_p)
    turn(act_t, act)
    for copy in later:
        copy.wait()


def out_kernel(act, w, bias, out):
    @pl.loop(0, w.shape[1] // 256)
    def _(i):
        at = pl.ds(pl.multiple_of(i * 256, 256), 256)
        out[:, at] = nn(act[...], w[:, at]) + bias[:, at]


def out_more_kernel(act, w, before, out):
    @pl.loop(0, w.shape[1] // 256)
    def _(i):
        at = pl.ds(pl.multiple_of(i * 256, 256), 256)
        out[:, at] = before[:, at] + nn(act[...], w[:, at])


def cot_kernel(out, *refs):
    pieces, (cot, total_ref) = refs[:-2], refs[-2:]
    z = lax.axis_index(Z)
    n = len(pieces)
    tokens = out.shape[0]
    lanes = pieces[0].shape[1]
    total_ref[...] = jnp.zeros_like(total_ref)
    step = 64

    def of(k):
        return pl.ds(pl.multiple_of(lax.rem(z - k + n, n) * lanes, lanes), lanes)

    @pl.loop(0, tokens // step)
    def _(i):
        at = pl.ds(pl.multiple_of(i * step, step), step)
        zz = yy = zy = jnp.zeros((step, lanes), f32)
        for k, piece in enumerate(pieces):
            o, t = out[at, of(k)], piece[at, :].astype(f32)
            zz, yy, zy = zz + o * o, yy + t * t, zy + o * t
        zz, yy, zy = (jnp.sum(v, axis=1, keepdims=True) for v in (zz, yy, zy))
        norm_z = jnp.sqrt(zz + epsilon)
        norms = norm_z * jnp.sqrt(yy + epsilon)
        cosine = zy / norms
        total_ref[...] += jnp.sum(cosine)
        by_target = 1.0 / norms
        by_out = cosine / (norm_z * norm_z)
        for k, piece in enumerate(pieces):
            o, t = out[at, of(k)], piece[at, :].astype(f32)
            cot[at, of(k)] = (by_out * o - t * by_target).astype(bf16)

    high, low = high_low(jnp.broadcast_to(total_ref[0:1, 0:1], (ROWS, cot.shape[1])))
    row = lax.broadcasted_iota(jnp.int32, high.shape, 0)
    cot[pl.ds(tokens, ROWS), :] = jnp.where(
        row == 0, high.astype(f32), jnp.where(row == 1, low.astype(f32), 0.0)
    ).astype(bf16)


def back_kernel(cot, w_mine, slope, dpre):
    @pl.loop(0, slope.shape[1] // 256)
    def _(i):
        at = pl.ds(pl.multiple_of(i * 256, 256), 256)
        dpre[:, at] = (nt(w_mine[...], cot[at, :]) * slope[:, at]).astype(bf16)


def small_rows(value, width):
    high, low = high_low(value)
    pad = width - 2 * value.shape[1]
    rest = [jnp.zeros((ROWS, pad), bf16)] if pad else []
    return jnp.concatenate([high, low] + rest, axis=1)


def small_value(rows, n):
    rows = rows.astype(f32)
    return rows[:, :n] + rows[:, n : 2 * n]


def grad_in_kernel(cot_p, w_mine, slope_p, dpre, rows, rows_p, m_a, m_b, m_c, own, own_bias, dpre_p):
    back_kernel(cot_p, w_mine, slope_p, dpre_p)
    block = dpre.shape[0] // (RING * RING)
    width = rows.shape[1]
    ones = jnp.ones((ROWS, rows.shape[0]), bf16)
    bias = nt(ones, dpre[...]) + nt(ones, dpre_p[...])

    turns = ((SHIFTS[0], m_a), (SHIFTS[1], m_b), (SHIFTS[2], m_c), (0, own))

    def columns(at):
        value = nn(dpre[...], rows[:, at]) + nn(dpre_p[...], rows_p[:, at])
        for k, to in turns:
            for kx in range(RING):
                part = value[(kx * RING + k) * block : (kx * RING + k + 1) * block]
                to[kx * block : (kx + 1) * block, at] = part.astype(to.dtype)

    whole = width // 256

    @pl.loop(0, whole)
    def _(j):
        columns(pl.ds(pl.multiple_of(j * 256, 256), 256))

    if whole * 256 < width:
        columns(slice(whole * 256, width))

    for k, to in turns:
        row = lax.broadcasted_iota(jnp.int32, (ROWS, 128), 0)
        small = jnp.zeros((ROWS, 128), f32)
        for kx in range(RING):
            at = (kx * RING + k) * block
            lane = at // 128 * 128
            part = bias[:, lane : lane + 128]
            if at != lane:
                part = jnp.concatenate([part[:, block:], part[:, :block]], axis=1)
            small = jnp.where(row == kx, part, small)
        if k:
            to[RING * block :, :] = small_rows(small, width)
        else:
            own_bias[...] = small


def grad_out_kernel(act, act_p, cot, cot_p, m_a, m_b, m_c, own, own_small):
    tokens = act.shape[1]
    step = 256

    @pl.loop(0, cot.shape[1] // step)
    def _(j):
        at = pl.ds(pl.multiple_of(j * step, step), step)
        value = nn(act[...], cot[0:tokens, at]) + nn(act_p[...], cot_p[0:tokens, at])
        for k, to in zip((*SHIFTS, 0), (m_a, m_b, m_c, own)):
            to[0:step, at] = value[k * step : (k + 1) * step].astype(to.dtype)

    def sums(ref):
        return jnp.sum(ref[0:tokens, :].astype(f32), axis=0, keepdims=True)

    def cosines(ref):
        tail = ref[tokens : tokens + ROWS, 0:128].astype(f32)
        return tail[0:1] + tail[1:2]

    bias = sums(cot) + sums(cot_p)
    loss = cosines(cot) + cosines(cot_p)
    row = lax.broadcasted_iota(jnp.int32, (ROWS, 128), 0)
    small = jnp.zeros((ROWS, 128), f32)
    for r in range(ROWS):
        small = jnp.where(row == r, bias[:, r * 128 : (r + 1) * 128], small)
    small = jnp.concatenate([small, jnp.broadcast_to(loss, (ROWS, 128))], axis=1)
    packed = small_rows(small, cot.shape[1])
    for to in (m_a, m_b, m_c):
        to[step:, :] = packed
    own_small[...] = small_value(packed, 256)


def middle_kernel(by_row, own, own_small, g_a, g_b, g_c, m_a, m_b, m_c, kept, kept_small):
    height = own.shape[0]
    block = height // RING
    width = own.shape[1]
    n = own_small.shape[1]
    got = (g_a, g_b, g_c)
    small = total(own_small[...], [small_value(g[height:, 0 : 2 * n], n) for g in got])
    packed = small_rows(small, width)
    for k, to in zip((*SHIFTS, 0), (m_a, m_b, m_c, kept)):
        at = pl.ds(k * block, block)
        value = total(own[at, :], [g[at, :].astype(f32) for g in got])
        to[0:block, :] = value.astype(to.dtype)
        if by_row:
            part = jnp.broadcast_to(small[k : k + 1], small.shape)
            if k:
                to[block:, :] = small_rows(part, width)
            else:
                kept_small[...] = part
        elif k:
            to[block:, :] = packed
        else:
            kept_small[...] = small_value(packed, n)


def joint_kernel(out_own, out_small, o2, o1, o3, in_own, in_small, i2, i1, i3, joint):
    block = out_own.shape[0]
    at = 0
    for own, got in ((out_own, (o2, o1, o3)), (in_own, (i2, i1, i3))):
        value = total(own[...], [g[0:block, :].astype(f32) for g in got]).astype(bf16)
        joint[:, :, at : at + own.shape[1]] = value.reshape(joint.shape[0], ROWS, -1)
        at += own.shape[1]
    for own, got in ((out_small, (o2, o1, o3)), (in_small, (i2, i1, i3))):
        n = own.shape[1]
        small = total(own[...], [small_value(g[block:, 0 : 2 * n], n) for g in got])
        packed = small_rows(small, 2 * n)
        for i in range(joint.shape[0]):
            joint[i, :, at : at + 2 * n] = packed
        at += 2 * n


def last_kernel(scale, width, channels, joint, grad_in, grad_out, bias_out, loss, bias_in):
    n = joint.shape[0]

    def along(lo, hi):
        value = joint[0, :, lo:hi].astype(f32)
        for i in range(1, n):
            value = value + joint[i, :, lo:hi].astype(f32)
        return value

    grad_out[...] = along(0, channels) * scale
    at = channels + width
    grad_in[...] = along(channels, at) * scale
    small = (along(at, at + 256) + along(at + 256, at + 512)) * scale
    bias_out[...] = small[:, 0:128]
    loss[...] = -small[:, 128:256]
    at += 512
    bias_in[...] = (along(at, at + 128) + along(at + 128, at + 256)) * scale


def turn_kernel(dpre_t, dpre_pt, dpre, dpre_p):
    turn(dpre_pt, dpre_p)
    turn(dpre_t, dpre)


def hidden_kernel(dpre, dpre_r, w_mine, w_other, grad):
    def columns(at):
        grad[:, at] = (nn(dpre[...], w_mine[:, at]) + nn(dpre_r[...], w_other[:, at])).astype(bf16)

    whole = grad.shape[1] // 256

    @pl.loop(0, whole)
    def _(i):
        columns(pl.ds(pl.multiple_of(i * 256, 256), 256))

    if whole * 256 < grad.shape[1]:
        columns(slice(whole * 256, grad.shape[1]))


def on_device(hidden_states, teacher, proj_in, bias_in, proj_out, bias_out):
    samples, seq, width = hidden_states.shape
    units, channels = proj_out.shape
    ny, nx, nc, nz = (lax.axis_size(a) for a in DP_FEAT)
    z = lax.axis_index(Z)
    tokens = samples * seq
    block = units // (ny * nx * nc)
    half = units // nc
    share = block // nz
    scale = 1.0 / float(tokens * ny * nx * nc * nz)
    sems = pltpu.SemaphoreType.DMA((RING * RING,))
    one = 2 * half * tokens * channels

    rows = hidden_states.reshape(tokens, width)
    rows_p = shift(rows, C, 1)

    pieces = {0: lax.dynamic_slice_in_dim(teacher, z * samples, samples, 0)}
    for k in (4, 3, 5, 2, 6, 1, 7):
        to = lax.rem(z + k, nz)
        piece = lax.dynamic_slice_in_dim(teacher, to * samples, samples, 0)
        pieces[k] = shift(piece, Z, k)
    pieces = [pieces[k].reshape(tokens, channels // nz) for k in range(nz)]

    w_in = proj_in.reshape(ny, nx, nc, block, width)
    w_out = proj_out.reshape(ny, nx, nc, block, channels)

    act_t, act_pt, slope, slope_p, act, act_p, in_mine, in_other, out_mine, out_other = call(
        first_kernel,
        [VMEM, VMEM, HBM, HBM, VMEM],
        [((half, tokens), bf16)] * 2
        + [((half, tokens), f32)] * 2
        + [((tokens, half), bf16)] * 2
        + [((half, width), bf16)] * 2
        + [((half, channels), bf16)] * 2,
        [pltpu.VMEM((half, 1), f32), sems, sems, sems, sems],
        2 * one,
        40,
    )(rows, rows_p, w_in, w_out, bias_in[:, None])
    act_r = shift(act_p, C, 1)
    big = ((tokens, channels), f32)
    (out,) = call(out_kernel, [VMEM] * 3, [big], (), one)(act, out_mine, bias_out[None])
    (out,) = call(out_more_kernel, [VMEM] * 3, [big], (), one)(act_r, out_other, out)

    (cot,) = call(
        cot_kernel,
        [VMEM] * (1 + nz),
        [((tokens + ROWS, channels), bf16)],
        [pltpu.VMEM((8, 128), f32)],
        one // 4,
    )(out, *pieces)
    cot_p = shift(cot, C, 1)
    (dpre_t,) = call(back_kernel, [VMEM] * 3, [((half, tokens), bf16)], (), one)(
        cot, out_mine, slope
    )

    def messages(height, wide):
        return [((height + ROWS, wide), bf16)] * 3 + [((height, wide), f32)]

    quarter = RING * block
    *first, first_own, first_small, dpre_pt = call(
        grad_in_kernel,
        [VMEM] * 6,
        messages(quarter, width) + [((ROWS, 128), f32), ((half, tokens), bf16)],
        (),
        3 * one,
    )(cot_p, out_mine, slope_p, dpre_t, rows, rows_p)
    first = [shift(m, Y, k) for m, k in zip(first, SHIFTS)]

    *last, last_own, last_small = call(
        grad_out_kernel, [VMEM] * 4, messages(quarter, channels) + [((ROWS, 256), f32)], (), 2 * one
    )(act_t, act_pt, cot, cot_p)
    last = [shift(m, X, k) for m, k in zip(last, SHIFTS)]

    dpre, dpre_p = call(
        turn_kernel, [VMEM] * 2, [((tokens, half), bf16)] * 2, (), one
    )(dpre_t, dpre_pt)
    dpre_r = shift(dpre_p, C, 1)

    *first, first_own, first_small = call(
        functools.partial(middle_kernel, True),
        [VMEM] * 5,
        messages(block, width) + [((ROWS, 128), f32)],
        (),
        one // 8,
    )(first_own, first_small, *first)
    first = [shift(m, X, k) for m, k in zip(first, SHIFTS)]
    *last, last_own, last_small = call(
        functools.partial(middle_kernel, False),
        [VMEM] * 5,
        messages(block, channels) + [((ROWS, 256), f32)],
        (),
        one // 8,
    )(last_own, last_small, *last)
    last = [shift(m, Y, k) for m, k in zip(last, SHIFTS)]

    (joint,) = call(
        joint_kernel, [VMEM] * 10, [((nz, share, channels + width + 768), bf16)], (), one // 8
    )(last_own, last_small, *last, first_own, first_small, *first)
    dpre_r, joint = lax.optimization_barrier((dpre_r, joint))
    joint = lax.all_to_all(joint, Z, split_axis=0, concat_axis=0, tiled=True)
    (grad_hidden,) = call(
        hidden_kernel, [VMEM] * 4, [((tokens, width), bf16)], (), 2 * one
    )(dpre, dpre_r, in_mine, in_other)
    grad_in, grad_out, grad_bias_out, loss, grad_bias_in = call(
        functools.partial(last_kernel, scale, width, channels),
        [VMEM],
        [((share, width), f32), ((share, channels), f32)] + [((ROWS, 128), f32)] * 3,
    )(joint)
    return (
        grad_in,
        lax.dynamic_slice_in_dim(grad_bias_in[0], z * share, share, 0),
        grad_out,
        grad_bias_out.reshape(channels),
        grad_hidden.reshape(samples, seq, width),
        loss[0, 0],
    )


def solution(mesh):
    finer = Mesh(mesh.devices.reshape(4, 4, 2, mesh.shape["feat"]), DP_FEAT)
    return jax.shard_map(
        on_device,
        mesh=finer,
        in_specs=(P(DP_FEAT, None, None), P(DP, None, Z), P(), P(), P(), P()),
        out_specs=(
            P(DP_FEAT, None),
            P(DP_FEAT),
            P(DP_FEAT, None),
            P(),
            P(DP_FEAT, None, None),
            P(),
        ),
        check_vma=False,
    )
```

```python
import functools

import jax
import jax.numpy as jnp
from jax import lax
from jax.experimental import pallas as pl
from jax.experimental.pallas import tpu as pltpu
from jax.sharding import Mesh
from jax.sharding import PartitionSpec as P


Y, X, C, Z = "dp_0", "dp_1", "dp_2", "feat"
DP = (Y, X, C)
DP_FEAT = (Y, X, C, Z)

epsilon = 1e-06
f32, bf16 = jnp.float32, jnp.bfloat16
RING = 4
SHIFTS = (2, 3, 1)
TEACH = (7, 1, 6, 2, 5, 3, 4)
ROWS = 8
MIB = 1 << 20

VMEM = pl.BlockSpec(memory_space=pltpu.VMEM)
HBM = pl.BlockSpec(memory_space=pltpu.HBM)


def shift(x, axis, k):
    n = lax.axis_size(axis)
    return lax.ppermute(x, axis, [(i, (i + k) % n) for i in range(n)])


def shifts(xs, axis):
    return [shift(x, axis, k) for x, k in zip(xs, SHIFTS)]


def nt(a, b):
    return lax.dot_general(a, b, (((1,), (1,)), ((), ())), preferred_element_type=f32)


def nn(a, b):
    return jnp.dot(a, b, preferred_element_type=f32)


def high_low(v):
    high = v.astype(bf16)
    return high, (v - high.astype(f32)).astype(bf16)


def total(own, got):
    at2, at3, at1 = got
    return (own + at2) + (at1 + at3)


def call(body, ins, outs, scratch=(), flops=0, limit=16):
    return pl.pallas_call(
        body,
        out_shape=[jax.ShapeDtypeStruct(s, d) for s, d in outs],
        in_specs=ins,
        out_specs=[VMEM] * len(outs),
        scratch_shapes=list(scratch),
        compiler_params=pltpu.CompilerParams(vmem_limit_bytes=limit * MIB),
        cost_estimate=pl.CostEstimate(flops=flops, bytes_accessed=4 * MIB, transcendentals=0),
    )


def in_hbm(x):
    return pltpu.with_memory_space_constraint(x, pltpu.HBM)


def gather(w_ref, to_ref, sem, core):
    y, x = lax.axis_index(Y), lax.axis_index(X)
    block = w_ref.shape[3]
    for kx in range(RING):
        for ky in range(RING):
            pltpu.make_async_copy(
                w_ref.at[lax.rem(y + ky, RING), lax.rem(x + kx, RING), core],
                to_ref.at[pl.ds((kx * RING + ky) * block, block)],
                sem,
            ).start()
    return pltpu.make_async_copy(to_ref, to_ref, sem)


def identity(n):
    row = lax.broadcasted_iota(jnp.int32, (n, n), 0)
    return jnp.where(row == lax.broadcasted_iota(jnp.int32, (n, n), 1), 1.0, 0.0).astype(bf16)


def turn(ref, to):
    eye = identity(256)

    for i in range(0, ref.shape[0], 256):
        for j in range(0, ref.shape[1], 256):
            to[j : j + 256, i : i + 256] = nt(eye, ref[i : i + 256, j : j + 256]).astype(bf16)


def first_kernel(
    rows, rows_p, w_in, w_out, bias, act_t, act_pt, slope, slope_p, act, act_p, out_mine,
    out_other, in_mine, col, s0, s1, s2,
):
    y, x, c = lax.axis_index(Y), lax.axis_index(X), lax.axis_index(C)
    now = gather(w_in, in_mine, s0, c)
    later = [gather(w_out, out_mine, s1, c), gather(w_out, out_other, s2, 1 - c)]
    block = w_in.shape[3]
    for kx in range(RING):
        for ky in range(RING):
            of = (lax.rem(y + ky, RING) * RING + lax.rem(x + kx, RING)) * 2 + c
            col[pl.ds((kx * RING + ky) * block, block), :] = bias[
                pl.ds(pl.multiple_of(of * block, block), block), :
            ]
    now.wait()

    for r, a, s in ((rows, act_t, slope), (rows_p, act_pt, slope_p)):

        @pl.loop(0, r.shape[0] // 256)
        def _(i):
            at = pl.ds(pl.multiple_of(i * 256, 256), 256)
            pre = nt(in_mine[...], r[at, :]) + col[...]
            sig = jax.nn.sigmoid(pre)
            a[:, at] = (pre * sig).astype(bf16)
            s[:, at] = sig * (1.0 + pre * (1.0 - sig))

    turn(act_pt, act_p)
    turn(act_t, act)
    for copy in later:
        copy.wait()


def out_kernel(act, w, bias, out):
    @pl.loop(0, w.shape[1] // 256)
    def _(i):
        at = pl.ds(pl.multiple_of(i * 256, 256), 256)
        out[:, at] = nn(act[...], w[:, at]) + bias[:, at]


def out_more_kernel(act, w, before, out):
    @pl.loop(0, w.shape[1] // 256)
    def _(i):
        at = pl.ds(pl.multiple_of(i * 256, 256), 256)
        out[:, at] = before[:, at] + nn(act[...], w[:, at])


def split_kernel(distances, teacher, *refs):
    outs, sems = refs[:-1], refs[-1]
    z, n = lax.axis_index(Z), lax.axis_size(Z)
    tokens = outs[0].shape[0]
    copies = []
    for i, (k, out) in enumerate(zip(distances, outs)):
        of = pl.multiple_of(lax.rem(z + k, n) * tokens, tokens)
        copies.append(pltpu.make_async_copy(teacher.at[pl.ds(of, tokens)], out, sems.at[i]))
    for copy in copies:
        copy.start()
    for copy in copies:
        copy.wait()


def cot_kernel(out, *refs):
    given, (cot, total_ref, held, sems) = refs[:-4], refs[-4:]
    z = lax.axis_index(Z)
    n = len(given)
    tokens = out.shape[0]
    lanes = given[0].shape[1]
    part = tokens // 2
    for p in range(2):
        for k, piece in enumerate(given):
            rows = pl.ds(p * part, part)
            if k == 0:
                rows = pl.ds(pl.multiple_of(z * tokens + p * part, part), part)
            pltpu.make_async_copy(piece.at[rows], held.at[p, k], sems.at[p]).start()
    total_ref[...] = jnp.zeros_like(total_ref)
    step = 64

    def of(k):
        return pl.ds(pl.multiple_of(lax.rem(z - k + n, n) * lanes, lanes), lanes)

    for p in range(2):
        pltpu.make_async_copy(held.at[p], held.at[p], sems.at[p]).wait()

        @pl.loop(0, part // step)
        def _(i):
            of_part = pl.ds(pl.multiple_of(i * step, step), step)
            at = pl.ds(pl.multiple_of(p * part + i * step, step), step)
            zz = yy = zy = jnp.zeros((step, lanes), f32)
            for k in range(n):
                o, t = out[at, of(k)], held[p, k, of_part, :].astype(f32)
                zz, yy, zy = zz + o * o, yy + t * t, zy + o * t
            zz, yy, zy = (jnp.sum(v, axis=1, keepdims=True) for v in (zz, yy, zy))
            norm_z = jnp.sqrt(zz + epsilon)
            norms = norm_z * jnp.sqrt(yy + epsilon)
            cosine = zy / norms
            total_ref[...] += jnp.sum(cosine)
            by_target = 1.0 / norms
            by_out = cosine / (norm_z * norm_z)
            for k in range(n):
                o, t = out[at, of(k)], held[p, k, of_part, :].astype(f32)
                cot[at, of(k)] = (by_out * o - t * by_target).astype(bf16)

    high, low = high_low(jnp.broadcast_to(total_ref[0:1, 0:1], (ROWS, cot.shape[1])))
    row = lax.broadcasted_iota(jnp.int32, high.shape, 0)
    cot[pl.ds(tokens, ROWS), :] = jnp.where(
        row == 0, high.astype(f32), jnp.where(row == 1, low.astype(f32), 0.0)
    ).astype(bf16)


def back_kernel(cot, w_mine, slope, dpre):
    @pl.loop(0, slope.shape[1] // 256)
    def _(i):
        at = pl.ds(pl.multiple_of(i * 256, 256), 256)
        dpre[:, at] = (nt(w_mine[...], cot[at, :]) * slope[:, at]).astype(bf16)


def small_rows(value, width):
    high, low = high_low(value)
    pad = width - 2 * value.shape[1]
    rest = [jnp.zeros((ROWS, pad), bf16)] if pad else []
    return jnp.concatenate([high, low] + rest, axis=1)


def small_value(rows, n):
    rows = rows.astype(f32)
    return rows[:, :n] + rows[:, n : 2 * n]


def with_ones(ref, width):
    return jnp.concatenate([ref[:, width - 128 :], jnp.ones((ref.shape[0], 128), bf16)], axis=1)


def over_columns(width, product, write):
    whole = (width - 128) // 256
    assert width == whole * 256 + 128

    @pl.loop(0, whole)
    def _(j):
        at = pl.ds(pl.multiple_of(j * 256, 256), 256)
        write(product(lambda ref: ref[:, at]), at)

    value = product(lambda ref: with_ones(ref, width))
    write(value[:, :128], slice(width - 128, width))
    return value[:, 128:]


def bias_rows(sums, block):
    row = lax.broadcasted_iota(jnp.int32, (ROWS, 128), 0)
    unit = lax.broadcasted_iota(jnp.int32, (block, 128), 0)
    lane = lax.broadcasted_iota(jnp.int32, (block, 128), 1)
    small = jnp.zeros((ROWS, 128), f32)
    for kx, part in enumerate(sums):
        part = jnp.sum(jnp.where(unit == lane, part, 0.0), axis=0, keepdims=True)
        small = jnp.where(row == kx, part, small)
    return small


def blocks_of(k, block):
    return [slice((kx * RING + k) * block, (kx * RING + k + 1) * block) for kx in range(RING)]


def grad_in_far_kernel(cot_p, w_mine, slope_p, dpre, rows, rows_p, far, mine, partner):
    block = dpre.shape[0] // (RING * RING)
    tokens, width = rows.shape
    of = blocks_of(SHIFTS[0], block)
    weights = jnp.concatenate([w_mine[b, :] for b in of], axis=0)
    mine[...] = jnp.concatenate([dpre[b, :] for b in of], axis=0)
    slope = jnp.concatenate([slope_p[b, :] for b in of], axis=0)
    partner[...] = (nt(weights, cot_p[0:tokens, :]) * slope).astype(bf16)

    def write(value, at):
        far[0 : RING * block, at] = value.astype(bf16)

    sums = over_columns(
        width, lambda take: nn(mine[...], take(rows)) + nn(partner[...], take(rows_p)), write
    )
    small = bias_rows([sums[i * block : (i + 1) * block] for i in range(RING)], block)
    far[RING * block :, :] = small_rows(small, width)


def grad_in_kernel(cot_p, w_mine, slope_p, dpre, rows, rows_p, m_b, m_c, own, own_bias, dpre_p):
    back_kernel(cot_p, w_mine, slope_p, dpre_p)
    block = dpre.shape[0] // (RING * RING)
    width = rows.shape[1]
    turns = ((SHIFTS[1], m_b), (SHIFTS[2], m_c), (0, own))

    def write(value, at):
        for k, to in turns:
            for kx, b in enumerate(blocks_of(k, block)):
                to[kx * block : (kx + 1) * block, at] = value[b].astype(to.dtype)

    sums = over_columns(
        width, lambda take: nn(dpre[...], take(rows)) + nn(dpre_p[...], take(rows_p)), write
    )
    for k, to in turns:
        small = bias_rows([sums[b] for b in blocks_of(k, block)], block)
        if k:
            to[RING * block :, :] = small_rows(small, width)
        else:
            own_bias[...] = small


def grad_out_far_kernel(act, act_p, cot, cot_p, far, packed, own_small):
    tokens = act.shape[1]
    step = 256
    units = slice(SHIFTS[0] * step, (SHIFTS[0] + 1) * step)

    @pl.loop(0, cot.shape[1] // step)
    def _(j):
        at = pl.ds(pl.multiple_of(j * step, step), step)
        value = nn(act[units, :], cot[0:tokens, at]) + nn(act_p[units, :], cot_p[0:tokens, at])
        far[0:step, at] = value.astype(bf16)

    def sums(ref):
        return jnp.sum(ref[0:tokens, :].astype(f32), axis=0, keepdims=True)

    def cosines(ref):
        tail = ref[tokens : tokens + ROWS, 0:128].astype(f32)
        return tail[0:1] + tail[1:2]

    bias = sums(cot) + sums(cot_p)
    loss = cosines(cot) + cosines(cot_p)
    row = lax.broadcasted_iota(jnp.int32, (ROWS, 128), 0)
    small = jnp.zeros((ROWS, 128), f32)
    for r in range(ROWS):
        small = jnp.where(row == r, bias[:, r * 128 : (r + 1) * 128], small)
    small = jnp.concatenate([small, jnp.broadcast_to(loss, (ROWS, 128))], axis=1)
    value = small_rows(small, cot.shape[1])
    far[step:, :] = value
    packed[...] = value
    own_small[...] = small_value(value, 256)


def grad_out_kernel(act, act_p, cot, cot_p, packed, m_b, m_c, own):
    tokens = act.shape[1]
    step = 256
    near = {k: to for k, to in zip((*SHIFTS[1:], 0), (m_b, m_c, own))}

    @pl.loop(0, cot.shape[1] // step)
    def _(j):
        at = pl.ds(pl.multiple_of(j * step, step), step)
        a, b = cot[0:tokens, at], cot_p[0:tokens, at]
        for low, high in ((0, 2), (3, 4)):
            units = slice(low * step, high * step)
            value = nn(act[units, :], a) + nn(act_p[units, :], b)
            for k in range(low, high):
                part = value[(k - low) * step : (k - low + 1) * step]
                near[k][0:step, at] = part.astype(near[k].dtype)

    for to in (m_b, m_c):
        to[step:, :] = packed[...]


def middle_kernel(by_row, own, own_small, g_a, g_b, g_c, m_a, m_b, m_c, kept, kept_small):
    height = own.shape[0]
    block = height // RING
    width = own.shape[1]
    n = own_small.shape[1]
    got = (g_a, g_b, g_c)
    small = total(own_small[...], [small_value(g[height:, 0 : 2 * n], n) for g in got])
    packed = small_rows(small, width)
    for k, to in zip((*SHIFTS, 0), (m_a, m_b, m_c, kept)):
        at = pl.ds(k * block, block)
        value = total(own[at, :], [g[at, :].astype(f32) for g in got])
        to[0:block, :] = value.astype(to.dtype)
        if by_row:
            part = jnp.broadcast_to(small[k : k + 1], small.shape)
            if k:
                to[block:, :] = small_rows(part, width)
            else:
                kept_small[...] = part
        elif k:
            to[block:, :] = packed
        else:
            kept_small[...] = small_value(packed, n)


def joint_kernel(out_own, out_small, o2, o1, o3, in_own, in_small, i2, i1, i3, joint):
    block = out_own.shape[0]
    at = 0
    for own, got in ((out_own, (o2, o1, o3)), (in_own, (i2, i1, i3))):
        value = total(own[...], [g[0:block, :].astype(f32) for g in got]).astype(bf16)
        joint[:, :, at : at + own.shape[1]] = value.reshape(joint.shape[0], ROWS, -1)
        at += own.shape[1]
    sums = []
    for own, got in ((out_small, (o2, o1, o3)), (in_small, (i2, i1, i3))):
        n = own.shape[1]
        sums.append(total(own[...], [small_value(g[block:, 0 : 2 * n], n) for g in got]))
    high, low = high_low(jnp.concatenate(sums, axis=1))
    row = lax.broadcasted_iota(jnp.int32, (ROWS, 128), 0)
    terms = [v[:, j : j + 128].astype(f32) for j in (256, 128) for v in (high, low)]
    mixed = jnp.where(row == 0, terms[0], terms[1])
    mixed = jnp.where(row == 2, terms[2], jnp.where(row == 3, terms[3], mixed))
    packed = jnp.concatenate([high[:, :128], low[:, :128], mixed.astype(bf16)], axis=1)
    for i in range(joint.shape[0]):
        joint[i, :, at:] = packed


def last_kernel(scale, width, channels, joint, grad_in, grad_out, bias_out, loss, bias_in):
    n = joint.shape[0]

    def along(lo, hi):
        value = joint[0, :, lo:hi].astype(f32)
        for i in range(1, n):
            value = value + joint[i, :, lo:hi].astype(f32)
        return value

    grad_out[...] = along(0, channels) * scale
    at = channels + width
    grad_in[...] = along(channels, at) * scale
    bias_out[...] = (along(at, at + 128) + along(at + 128, at + 256)) * scale
    mixed = along(at + 256, at + 384) * scale
    loss[...] = -(mixed[2:3, 0:1] + mixed[3:4, 0:1])
    share = bias_in.shape[1]
    back = lax.rem(128 - lax.axis_index(Z) * share, 128)
    both = jnp.broadcast_to(mixed[0:1] + mixed[1:2], (ROWS, 128))
    bias_in[...] = pltpu.roll(both, back, 1)[0:1, :share]


def turn_kernel(dpre_t, dpre_pt, dpre, dpre_p):
    turn(dpre_pt, dpre_p)
    turn(dpre_t, dpre)


def hidden_kernel(dpre, dpre_r, w, grad, w_mine, w_other, s0, s1):
    c = lax.axis_index(C)
    copies = [gather(w, w_mine, s0, c), gather(w, w_other, s1, 1 - c)]
    for copy in copies:
        copy.wait()

    def columns(at):
        grad[:, at] = (nn(dpre[...], w_mine[:, at]) + nn(dpre_r[...], w_other[:, at])).astype(bf16)

    whole = grad.shape[1] // 256

    @pl.loop(0, whole)
    def _(i):
        columns(pl.ds(pl.multiple_of(i * 256, 256), 256))

    if whole * 256 < grad.shape[1]:
        columns(slice(whole * 256, grad.shape[1]))


def on_device(hidden_states, teacher, proj_in, bias_in, proj_out, bias_out):
    samples, seq, width = hidden_states.shape
    units, channels = proj_out.shape
    ny, nx, nc, nz = (lax.axis_size(a) for a in DP_FEAT)
    tokens = samples * seq
    block = units // (ny * nx * nc)
    half = units // nc
    share = block // nz
    scale = 1.0 / float(tokens * ny * nx * nc * nz)
    sems = pltpu.SemaphoreType.DMA
    one = 2 * half * tokens * channels

    rows = hidden_states.reshape(tokens, width)
    rows_p = shift(rows, C, 1)

    channel_rows = in_hbm(teacher.reshape(nz * tokens, channels // nz))
    pieces = [channel_rows] + [None] * (nz - 1)
    parts = call(
        functools.partial(split_kernel, TEACH),
        [HBM],
        [((tokens, channels // nz), bf16)] * len(TEACH),
        [pltpu.SemaphoreType.DMA((len(TEACH),))],
        limit=4,
    )(channel_rows)
    for k, part in zip(TEACH, parts):
        pieces[k] = shift(part, Z, k)

    w_in = in_hbm(proj_in.reshape(ny, nx, nc, block, width))
    w_out = in_hbm(proj_out.reshape(ny, nx, nc, block, channels))

    act_t, act_pt, slope, slope_p, act, act_p, out_mine, out_other = call(
        first_kernel,
        [VMEM, VMEM, HBM, HBM, VMEM],
        [((half, tokens), bf16)] * 2
        + [((half, tokens), f32)] * 2
        + [((tokens, half), bf16)] * 2
        + [((half, channels), bf16)] * 2,
        [pltpu.VMEM((half, width), bf16), pltpu.VMEM((half, 1), f32), sems, sems, sems],
        2 * one,
        12,
    )(rows, rows_p, w_in, w_out, bias_in[:, None])
    act_r = shift(act_p, C, 1)
    big = ((tokens, channels), f32)
    (out,) = call(out_kernel, [VMEM] * 3, [big], (), one)(act, out_mine, bias_out[None])
    (out,) = call(out_more_kernel, [VMEM] * 3, [big], (), one)(act_r, out_other, out)

    (cot,) = call(
        cot_kernel,
        [VMEM] + [HBM] * nz,
        [((tokens + ROWS, channels), bf16)],
        [
            pltpu.VMEM((8, 128), f32),
            pltpu.VMEM((2, nz, tokens // 2, channels // nz), bf16),
            pltpu.SemaphoreType.DMA((2,)),
        ],
        one // 4,
    )(out, channel_rows, *map(in_hbm, pieces[1:]))
    cot_p = shift(cot, C, 1)
    (dpre_t,) = call(back_kernel, [VMEM] * 3, [((half, tokens), bf16)], (), one)(
        cot, out_mine, slope
    )

    def messages(height, wide):
        return [((height + ROWS, wide), bf16)] * 3 + [((height, wide), f32)]

    quarter = RING * block
    inputs = (cot_p, out_mine, slope_p, dpre_t, rows, rows_p)
    (far,) = call(
        grad_in_far_kernel,
        [VMEM] * 6,
        messages(quarter, width)[:1],
        [pltpu.VMEM((quarter, tokens), bf16)] * 2,
        one,
    )(*inputs)
    *near, first_own, first_small, dpre_pt = call(
        grad_in_kernel,
        [VMEM] * 6,
        messages(quarter, width)[1:] + [((ROWS, 128), f32), ((half, tokens), bf16)],
        (),
        3 * one,
    )(*inputs)
    first = shifts((far, *near), Y)

    inputs = (act_t, act_pt, cot, cot_p)
    far, packed, last_small = call(
        grad_out_far_kernel,
        [VMEM] * 4,
        messages(quarter, channels)[:1] + [((ROWS, channels), bf16), ((ROWS, 256), f32)],
        (),
        one // 2,
    )(*inputs)
    *near, last_own = call(
        grad_out_kernel, [VMEM] * 5, messages(quarter, channels)[1:], (), 2 * one
    )(*inputs, packed)
    last = shifts((far, *near), X)

    dpre, dpre_p = call(
        turn_kernel, [VMEM] * 2, [((tokens, half), bf16)] * 2, (), one
    )(dpre_t, dpre_pt)
    dpre_r = shift(dpre_p, C, 1)

    *first, first_own, first_small = call(
        functools.partial(middle_kernel, True),
        [VMEM] * 5,
        messages(block, width) + [((ROWS, 128), f32)],
        (),
        one // 8,
    )(first_own, first_small, *first)
    first = shifts(first, X)
    *last, last_own, last_small = call(
        functools.partial(middle_kernel, False),
        [VMEM] * 5,
        messages(block, channels) + [((ROWS, 256), f32)],
        (),
        one // 8,
    )(last_own, last_small, *last)
    last = shifts(last, Y)

    (joint,) = call(
        joint_kernel, [VMEM] * 10, [((nz, share, channels + width + 384), bf16)], (), one // 8
    )(last_own, last_small, *last, first_own, first_small, *first)
    dpre_r, joint = lax.optimization_barrier((dpre_r, joint))
    joint = lax.all_to_all(joint, Z, split_axis=0, concat_axis=0, tiled=True)
    (grad_hidden,) = call(
        hidden_kernel,
        [VMEM, VMEM, HBM],
        [((tokens, width), bf16)],
        [pltpu.VMEM((half, width), bf16)] * 2 + [sems, sems],
        2 * one,
        20,
    )(dpre, dpre_r, w_in)
    grad_in, grad_out, grad_bias_out, loss, grad_bias_in = call(
        functools.partial(last_kernel, scale, width, channels),
        [VMEM],
        [((share, width), f32), ((share, channels), f32), ((ROWS, 128), f32)]
        + [((1, 1), f32), ((1, share), f32)],
    )(joint)
    return (
        grad_in,
        grad_bias_in.reshape(share),
        grad_out,
        grad_bias_out.reshape(channels),
        grad_hidden.reshape(samples, seq, width),
        loss.reshape(()),
    )


def solution(mesh):
    finer = Mesh(mesh.devices.reshape(4, 4, 2, mesh.shape["feat"]), DP_FEAT)
    return jax.shard_map(
        on_device,
        mesh=finer,
        in_specs=(P(DP_FEAT, None, None), P(DP, None, Z), P(), P(), P(), P()),
        out_specs=(
            P(DP_FEAT, None),
            P(DP_FEAT),
            P(DP_FEAT, None),
            P(),
            P(DP_FEAT, None, None),
            P(),
        ),
        check_vma=False,
    )
```

```python
import functools

import jax
import jax.numpy as jnp
from jax import lax
from jax.experimental import pallas as pl
from jax.experimental.pallas import tpu as pltpu
from jax.sharding import Mesh
from jax.sharding import PartitionSpec as P


Y, X, C, Z = "dp_0", "dp_1", "dp_2", "feat"
DP = (Y, X, C)
DP_FEAT = (Y, X, C, Z)

epsilon = 1e-06
f32, bf16 = jnp.float32, jnp.bfloat16
RING = 4
SHIFTS = (2, 3, 1)
TEACH = (7, 1, 6, 2, 5, 3, 4)
ROWS = 8
MIB = 1 << 20

VMEM = pl.BlockSpec(memory_space=pltpu.VMEM)
HBM = pl.BlockSpec(memory_space=pltpu.HBM)


def shift(x, axis, k):
    n = lax.axis_size(axis)
    return lax.ppermute(x, axis, [(i, (i + k) % n) for i in range(n)])


def shifts(xs, axis):
    return [shift(x, axis, k) for x, k in zip(xs, SHIFTS)]


def nt(a, b):
    return lax.dot_general(a, b, (((1,), (1,)), ((), ())), preferred_element_type=f32)


def nn(a, b):
    return jnp.dot(a, b, preferred_element_type=f32)


def high_low(v):
    high = v.astype(bf16)
    return high, (v - high.astype(f32)).astype(bf16)


def total(own, got):
    at2, at3, at1 = got
    return (own + at2) + (at1 + at3)


def call(body, ins, outs, scratch=(), flops=0, limit=16):
    return pl.pallas_call(
        body,
        out_shape=[jax.ShapeDtypeStruct(s, d) for s, d in outs],
        in_specs=ins,
        out_specs=[VMEM] * len(outs),
        scratch_shapes=list(scratch),
        compiler_params=pltpu.CompilerParams(vmem_limit_bytes=limit * MIB),
        cost_estimate=pl.CostEstimate(flops=flops, bytes_accessed=4 * MIB, transcendentals=0),
    )


def in_hbm(x):
    return pltpu.with_memory_space_constraint(x, pltpu.HBM)


def gather(w_ref, to_ref, sem, core):
    y, x = lax.axis_index(Y), lax.axis_index(X)
    block = w_ref.shape[3]
    for kx in range(RING):
        for ky in range(RING):
            pltpu.make_async_copy(
                w_ref.at[lax.rem(y + ky, RING), lax.rem(x + kx, RING), core],
                to_ref.at[pl.ds((kx * RING + ky) * block, block)],
                sem,
            ).start()
    return pltpu.make_async_copy(to_ref, to_ref, sem)


def identity(n):
    row = lax.broadcasted_iota(jnp.int32, (n, n), 0)
    return jnp.where(row == lax.broadcasted_iota(jnp.int32, (n, n), 1), 1.0, 0.0).astype(bf16)


def turn(ref, to):
    eye = identity(256)

    for i in range(0, ref.shape[0], 256):
        for j in range(0, ref.shape[1], 256):
            to[j : j + 256, i : i + 256] = nt(eye, ref[i : i + 256, j : j + 256]).astype(bf16)


def first_kernel(
    rows_hbm, rows_p, w_in, w_out, bias_hbm, act_t, act_pt, slope, slope_p, act, act_p, out_mine,
    out_other, in_mine, rows, bias, col, s0, s1, s2, s3,
):
    y, x, c = lax.axis_index(Y), lax.axis_index(X), lax.axis_index(C)
    bias_copy = pltpu.make_async_copy(bias_hbm, bias, s3.at[0])
    rows_copy = pltpu.make_async_copy(rows_hbm, rows, s3.at[1])
    bias_copy.start()
    now = gather(w_in, in_mine, s0, c)
    rows_copy.start()
    later = [gather(w_out, out_mine, s1, c), gather(w_out, out_other, s2, 1 - c)]
    block = w_in.shape[3]
    unit = lax.broadcasted_iota(jnp.int32, (block, bias.shape[1]), 0)
    lane = lax.broadcasted_iota(jnp.int32, (block, bias.shape[1]), 1)
    ours = lane == unit + c * block
    bias_copy.wait()
    for kx in range(RING):
        for ky in range(RING):
            of = lax.rem(y + ky, RING) * RING + lax.rem(x + kx, RING)
            terms = jnp.where(ours, bias[pl.ds(of, 1), :], 0.0)
            col[pl.ds((kx * RING + ky) * block, block), :] = jnp.sum(terms, axis=1, keepdims=True)
    now.wait()
    rows_copy.wait()

    for r, a, s in ((rows, act_t, slope), (rows_p, act_pt, slope_p)):

        @pl.loop(0, r.shape[0] // 256)
        def _(i):
            at = pl.ds(pl.multiple_of(i * 256, 256), 256)
            pre = nt(in_mine[...], r[at, :]) + col[...]
            sig = jax.nn.sigmoid(pre)
            a[:, at] = (pre * sig).astype(bf16)
            s[:, at] = sig * (1.0 + pre * (1.0 - sig))

    turn(act_pt, act_p)
    turn(act_t, act)
    for copy in later:
        copy.wait()


def out_kernel(act, w, bias, out):
    @pl.loop(0, w.shape[1] // 256)
    def _(i):
        at = pl.ds(pl.multiple_of(i * 256, 256), 256)
        out[:, at] = nn(act[...], w[:, at]) + bias[:, at]


def out_more_kernel(act, w, before, out):
    @pl.loop(0, w.shape[1] // 256)
    def _(i):
        at = pl.ds(pl.multiple_of(i * 256, 256), 256)
        out[:, at] = before[:, at] + nn(act[...], w[:, at])


def split_kernel(distances, teacher, *refs):
    outs, sems = refs[:-1], refs[-1]
    z, n = lax.axis_index(Z), lax.axis_size(Z)
    tokens = outs[0].shape[0]
    copies = []
    for i, (k, out) in enumerate(zip(distances, outs)):
        of = pl.multiple_of(lax.rem(z + k, n) * tokens, tokens)
        copies.append(pltpu.make_async_copy(teacher.at[pl.ds(of, tokens)], out, sems.at[i]))
    for copy in copies:
        copy.start()
    for copy in copies:
        copy.wait()


def cot_kernel(out, *refs):
    pieces, (cot, total_ref) = refs[:-2], refs[-2:]
    z = lax.axis_index(Z)
    n = len(pieces)
    tokens = out.shape[0]
    lanes = pieces[0].shape[1]
    total_ref[...] = jnp.zeros_like(total_ref)
    step = 64

    def of(k):
        return pl.ds(pl.multiple_of(lax.rem(z - k + n, n) * lanes, lanes), lanes)

    @pl.loop(0, tokens // step)
    def _(i):
        at = pl.ds(pl.multiple_of(i * step, step), step)
        zz = yy = zy = jnp.zeros((step, lanes), f32)
        for k, piece in enumerate(pieces):
            o, t = out[at, of(k)], piece[at, :].astype(f32)
            zz, yy, zy = zz + o * o, yy + t * t, zy + o * t
        zz, yy, zy = (jnp.sum(v, axis=1, keepdims=True) for v in (zz, yy, zy))
        norm_z = jnp.sqrt(zz + epsilon)
        norms = norm_z * jnp.sqrt(yy + epsilon)
        cosine = zy / norms
        total_ref[...] += jnp.sum(cosine)
        by_target = 1.0 / norms
        by_out = cosine / (norm_z * norm_z)
        for k, piece in enumerate(pieces):
            o, t = out[at, of(k)], piece[at, :].astype(f32)
            cot[at, of(k)] = (by_out * o - t * by_target).astype(bf16)

    high, low = high_low(jnp.broadcast_to(total_ref[0:1, 0:1], (ROWS, cot.shape[1])))
    row = lax.broadcasted_iota(jnp.int32, high.shape, 0)
    cot[pl.ds(tokens, ROWS), :] = jnp.where(
        row == 0, high.astype(f32), jnp.where(row == 1, low.astype(f32), 0.0)
    ).astype(bf16)


def back_kernel(cot, w_mine, slope, dpre):
    @pl.loop(0, slope.shape[1] // 256)
    def _(i):
        at = pl.ds(pl.multiple_of(i * 256, 256), 256)
        dpre[:, at] = (nt(w_mine[...], cot[at, :]) * slope[:, at]).astype(bf16)


def small_rows(value, width):
    high, low = high_low(value)
    pad = width - 2 * value.shape[1]
    rest = [jnp.zeros((ROWS, pad), bf16)] if pad else []
    return jnp.concatenate([high, low] + rest, axis=1)


def small_value(rows, n):
    rows = rows.astype(f32)
    return rows[:, :n] + rows[:, n : 2 * n]


def with_ones(ref, width):
    return jnp.concatenate([ref[:, width - 128 :], jnp.ones((ref.shape[0], 128), bf16)], axis=1)


def over_columns(width, product, write):
    whole = (width - 128) // 256
    assert width == whole * 256 + 128

    @pl.loop(0, whole)
    def _(j):
        at = pl.ds(pl.multiple_of(j * 256, 256), 256)
        write(product(lambda ref: ref[:, at]), at)

    value = product(lambda ref: with_ones(ref, width))
    write(value[:, :128], slice(width - 128, width))
    return value[:, 128:]


def bias_rows(sums, block):
    row = lax.broadcasted_iota(jnp.int32, (ROWS, 128), 0)
    unit = lax.broadcasted_iota(jnp.int32, (block, 128), 0)
    lane = lax.broadcasted_iota(jnp.int32, (block, 128), 1)
    small = jnp.zeros((ROWS, 128), f32)
    for kx, part in enumerate(sums):
        part = jnp.sum(jnp.where(unit == lane, part, 0.0), axis=0, keepdims=True)
        small = jnp.where(row == kx, part, small)
    return small


def blocks_of(k, block):
    return [slice((kx * RING + k) * block, (kx * RING + k + 1) * block) for kx in range(RING)]


def grad_in_far_kernel(cot_p, w_mine, slope_p, dpre, rows, rows_p, far, mine, partner):
    block = dpre.shape[0] // (RING * RING)
    tokens, width = rows.shape
    of = blocks_of(SHIFTS[0], block)
    weights = jnp.concatenate([w_mine[b, :] for b in of], axis=0)
    mine[...] = jnp.concatenate([dpre[b, :] for b in of], axis=0)
    slope = jnp.concatenate([slope_p[b, :] for b in of], axis=0)
    partner[...] = (nt(weights, cot_p[0:tokens, :]) * slope).astype(bf16)

    def write(value, at):
        far[0 : RING * block, at] = value.astype(bf16)

    sums = over_columns(
        width, lambda take: nn(mine[...], take(rows)) + nn(partner[...], take(rows_p)), write
    )
    small = bias_rows([sums[i * block : (i + 1) * block] for i in range(RING)], block)
    far[RING * block :, :] = small_rows(small, width)


def grad_in_kernel(cot_p, w_mine, slope_p, dpre, rows, rows_p, m_b, m_c, own, own_bias, dpre_p):
    back_kernel(cot_p, w_mine, slope_p, dpre_p)
    block = dpre.shape[0] // (RING * RING)
    width = rows.shape[1]
    turns = ((SHIFTS[1], m_b), (SHIFTS[2], m_c), (0, own))

    def write(value, at):
        for k, to in turns:
            for kx, b in enumerate(blocks_of(k, block)):
                to[kx * block : (kx + 1) * block, at] = value[b].astype(to.dtype)

    sums = over_columns(
        width, lambda take: nn(dpre[...], take(rows)) + nn(dpre_p[...], take(rows_p)), write
    )
    for k, to in turns:
        small = bias_rows([sums[b] for b in blocks_of(k, block)], block)
        if k:
            to[RING * block :, :] = small_rows(small, width)
        else:
            own_bias[...] = small


def grad_out_far_kernel(act, act_p, cot, cot_p, far, packed, own_small):
    tokens = act.shape[1]
    step = 256
    units = slice(SHIFTS[0] * step, (SHIFTS[0] + 1) * step)

    @pl.loop(0, cot.shape[1] // step)
    def _(j):
        at = pl.ds(pl.multiple_of(j * step, step), step)
        value = nn(act[units, :], cot[0:tokens, at]) + nn(act_p[units, :], cot_p[0:tokens, at])
        far[0:step, at] = value.astype(bf16)

    def sums(ref):
        return jnp.sum(ref[0:tokens, :].astype(f32), axis=0, keepdims=True)

    def cosines(ref):
        tail = ref[tokens : tokens + ROWS, 0:128].astype(f32)
        return tail[0:1] + tail[1:2]

    bias = sums(cot) + sums(cot_p)
    loss = cosines(cot) + cosines(cot_p)
    row = lax.broadcasted_iota(jnp.int32, (ROWS, 128), 0)
    small = jnp.zeros((ROWS, 128), f32)
    for r in range(ROWS):
        small = jnp.where(row == r, bias[:, r * 128 : (r + 1) * 128], small)
    small = jnp.concatenate([small, jnp.broadcast_to(loss, (ROWS, 128))], axis=1)
    value = small_rows(small, cot.shape[1])
    far[step:, :] = value
    packed[...] = value
    own_small[...] = small_value(value, 256)


def grad_out_kernel(act, act_p, cot, cot_p, packed, m_b, m_c, own):
    tokens = act.shape[1]
    step = 256
    near = {k: to for k, to in zip((*SHIFTS[1:], 0), (m_b, m_c, own))}

    @pl.loop(0, cot.shape[1] // step)
    def _(j):
        at = pl.ds(pl.multiple_of(j * step, step), step)
        a, b = cot[0:tokens, at], cot_p[0:tokens, at]
        for low, high in ((0, 2), (3, 4)):
            units = slice(low * step, high * step)
            value = nn(act[units, :], a) + nn(act_p[units, :], b)
            for k in range(low, high):
                part = value[(k - low) * step : (k - low + 1) * step]
                near[k][0:step, at] = part.astype(near[k].dtype)

    for to in (m_b, m_c):
        to[step:, :] = packed[...]


def middle_kernel(by_row, own, own_small, g_a, g_b, g_c, m_a, m_b, m_c, kept, kept_small):
    height = own.shape[0]
    block = height // RING
    width = own.shape[1]
    n = own_small.shape[1]
    got = (g_a, g_b, g_c)
    small = total(own_small[...], [small_value(g[height:, 0 : 2 * n], n) for g in got])
    packed = small_rows(small, width)
    for k, to in zip((*SHIFTS, 0), (m_a, m_b, m_c, kept)):
        at = pl.ds(k * block, block)
        value = total(own[at, :], [g[at, :].astype(f32) for g in got])
        to[0:block, :] = value.astype(to.dtype)
        if by_row:
            part = jnp.broadcast_to(small[k : k + 1], small.shape)
            if k:
                to[block:, :] = small_rows(part, width)
            else:
                kept_small[...] = part
        elif k:
            to[block:, :] = packed
        else:
            kept_small[...] = small_value(packed, n)


def joint_kernel(out_own, out_small, o2, o1, o3, in_own, in_small, i2, i1, i3, joint):
    block = out_own.shape[0]
    at = 0
    for own, got in ((out_own, (o2, o1, o3)), (in_own, (i2, i1, i3))):
        value = total(own[...], [g[0:block, :].astype(f32) for g in got]).astype(bf16)
        joint[:, :, at : at + own.shape[1]] = value.reshape(joint.shape[0], ROWS, -1)
        at += own.shape[1]
    sums = []
    for own, got in ((out_small, (o2, o1, o3)), (in_small, (i2, i1, i3))):
        n = own.shape[1]
        sums.append(total(own[...], [small_value(g[block:, 0 : 2 * n], n) for g in got]))
    high, low = high_low(jnp.concatenate(sums, axis=1))
    row = lax.broadcasted_iota(jnp.int32, (ROWS, 128), 0)
    terms = [v[:, j : j + 128].astype(f32) for j in (256, 128) for v in (high, low)]
    mixed = jnp.where(row == 0, terms[0], terms[1])
    mixed = jnp.where(row == 2, terms[2], jnp.where(row == 3, terms[3], mixed))
    packed = jnp.concatenate([high[:, :128], low[:, :128], mixed.astype(bf16)], axis=1)
    for i in range(joint.shape[0]):
        joint[i, :, at:] = packed


def last_kernel(scale, width, channels, joint, grad_in, grad_out, bias_out, loss, bias_in):
    n = joint.shape[0]

    def along(lo, hi):
        value = joint[0, :, lo:hi].astype(f32)
        for i in range(1, n):
            value = value + joint[i, :, lo:hi].astype(f32)
        return value

    grad_out[...] = along(0, channels) * scale
    at = channels + width
    grad_in[...] = along(channels, at) * scale
    bias_out[...] = (along(at, at + 128) + along(at + 128, at + 256)) * scale
    mixed = along(at + 256, at + 384) * scale
    loss[...] = -(mixed[2:3, 0:1] + mixed[3:4, 0:1])
    share = bias_in.shape[1]
    back = lax.rem(128 - lax.axis_index(Z) * share, 128)
    both = jnp.broadcast_to(mixed[0:1] + mixed[1:2], (ROWS, 128))
    bias_in[...] = pltpu.roll(both, back, 1)[0:1, :share]


def turn_kernel(dpre_t, dpre_pt, dpre, dpre_p):
    turn(dpre_pt, dpre_p)
    turn(dpre_t, dpre)


def hidden_kernel(dpre, dpre_r, w, grad, w_mine, w_other, s0, s1):
    c = lax.axis_index(C)
    copies = [gather(w, w_mine, s0, c), gather(w, w_other, s1, 1 - c)]
    for copy in copies:
        copy.wait()

    def columns(at):
        grad[:, at] = (nn(dpre[...], w_mine[:, at]) + nn(dpre_r[...], w_other[:, at])).astype(bf16)

    whole = grad.shape[1] // 256

    @pl.loop(0, whole)
    def _(i):
        columns(pl.ds(pl.multiple_of(i * 256, 256), 256))

    if whole * 256 < grad.shape[1]:
        columns(slice(whole * 256, grad.shape[1]))


def on_device(hidden_states, teacher, proj_in, bias_in, proj_out, bias_out):
    samples, seq, width = hidden_states.shape
    units, channels = proj_out.shape
    ny, nx, nc, nz = (lax.axis_size(a) for a in DP_FEAT)
    tokens = samples * seq
    block = units // (ny * nx * nc)
    half = units // nc
    share = block // nz
    scale = 1.0 / float(tokens * ny * nx * nc * nz)
    sems = pltpu.SemaphoreType.DMA
    one = 2 * half * tokens * channels

    rows = hidden_states.reshape(tokens, width)
    rows_p = shift(rows, C, 1)

    channel_rows = in_hbm(teacher.reshape(nz * tokens, channels // nz))
    parts = call(
        functools.partial(split_kernel, (*TEACH, 0)),
        [HBM],
        [((tokens, channels // nz), bf16)] * nz,
        [pltpu.SemaphoreType.DMA((nz,))],
        limit=4,
    )(channel_rows)
    pieces = [parts[-1]] + [None] * (nz - 1)
    for k, part in zip(TEACH, parts):
        pieces[k] = shift(part, Z, k)

    w_in = in_hbm(proj_in.reshape(ny, nx, nc, block, width))
    w_out = in_hbm(proj_out.reshape(ny, nx, nc, block, channels))

    act_t, act_pt, slope, slope_p, act, act_p, out_mine, out_other = call(
        first_kernel,
        [HBM, VMEM, HBM, HBM, HBM],
        [((half, tokens), bf16)] * 2
        + [((half, tokens), f32)] * 2
        + [((tokens, half), bf16)] * 2
        + [((half, channels), bf16)] * 2,
        [
            pltpu.VMEM((half, width), bf16),
            pltpu.VMEM((tokens, width), bf16),
            pltpu.VMEM((ny * nx, nc * block), f32),
            pltpu.VMEM((half, 1), f32),
            sems,
            sems,
            sems,
            pltpu.SemaphoreType.DMA((2,)),
        ],
        2 * one,
        12,
    )(in_hbm(rows), rows_p, w_in, w_out, in_hbm(bias_in.reshape(ny * nx, nc * block)))
    act_r = shift(act_p, C, 1)
    big = ((tokens, channels), f32)
    (out,) = call(out_kernel, [VMEM] * 3, [big], (), one)(act, out_mine, bias_out[None])
    (out,) = call(out_more_kernel, [VMEM] * 3, [big], (), one)(act_r, out_other, out)

    (cot,) = call(
        cot_kernel,
        [VMEM] * (1 + nz),
        [((tokens + ROWS, channels), bf16)],
        [pltpu.VMEM((8, 128), f32)],
        one // 4,
    )(out, *pieces)
    cot_p = shift(cot, C, 1)
    (dpre_t,) = call(back_kernel, [VMEM] * 3, [((half, tokens), bf16)], (), one)(
        cot, out_mine, slope
    )

    def messages(height, wide):
        return [((height + ROWS, wide), bf16)] * 3 + [((height, wide), f32)]

    quarter = RING * block
    inputs = (cot_p, out_mine, slope_p, dpre_t, rows, rows_p)
    (far,) = call(
        grad_in_far_kernel,
        [VMEM] * 6,
        messages(quarter, width)[:1],
        [pltpu.VMEM((quarter, tokens), bf16)] * 2,
        one,
    )(*inputs)
    *near, first_own, first_small, dpre_pt = call(
        grad_in_kernel,
        [VMEM] * 6,
        messages(quarter, width)[1:] + [((ROWS, 128), f32), ((half, tokens), bf16)],
        (),
        3 * one,
    )(*inputs)
    first = shifts((far, *near), Y)

    inputs = (act_t, act_pt, cot, cot_p)
    far, packed, last_small = call(
        grad_out_far_kernel,
        [VMEM] * 4,
        messages(quarter, channels)[:1] + [((ROWS, channels), bf16), ((ROWS, 256), f32)],
        (),
        one // 2,
    )(*inputs)
    *near, last_own = call(
        grad_out_kernel, [VMEM] * 5, messages(quarter, channels)[1:], (), 2 * one
    )(*inputs, packed)
    last = shifts((far, *near), X)

    dpre, dpre_p = call(
        turn_kernel, [VMEM] * 2, [((tokens, half), bf16)] * 2, (), one
    )(dpre_t, dpre_pt)
    dpre_r = shift(dpre_p, C, 1)

    *first, first_own, first_small = call(
        functools.partial(middle_kernel, True),
        [VMEM] * 5,
        messages(block, width) + [((ROWS, 128), f32)],
        (),
        one // 8,
    )(first_own, first_small, *first)
    first = shifts(first, X)
    *last, last_own, last_small = call(
        functools.partial(middle_kernel, False),
        [VMEM] * 5,
        messages(block, channels) + [((ROWS, 256), f32)],
        (),
        one // 8,
    )(last_own, last_small, *last)
    last = shifts(last, Y)

    (joint,) = call(
        joint_kernel, [VMEM] * 10, [((nz, share, channels + width + 384), bf16)], (), one // 8
    )(last_own, last_small, *last, first_own, first_small, *first)
    joint = lax.all_to_all(joint, Z, split_axis=0, concat_axis=0, tiled=True)
    (grad_hidden,) = call(
        hidden_kernel,
        [VMEM, VMEM, HBM],
        [((tokens, width), bf16)],
        [pltpu.VMEM((half, width), bf16)] * 2 + [sems, sems],
        2 * one,
        20,
    )(dpre, dpre_r, w_in)
    grad_in, grad_out, grad_bias_out, loss, grad_bias_in = call(
        functools.partial(last_kernel, scale, width, channels),
        [VMEM],
        [((share, width), f32), ((share, channels), f32), ((ROWS, 128), f32)]
        + [((1, 1), f32), ((1, share), f32)],
    )(joint)
    return (
        grad_in,
        grad_bias_in.reshape(share),
        grad_out,
        grad_bias_out.reshape(channels),
        grad_hidden.reshape(samples, seq, width),
        loss.reshape(()),
    )


def solution(mesh):
    finer = Mesh(mesh.devices.reshape(4, 4, 2, mesh.shape["feat"]), DP_FEAT)
    return jax.shard_map(
        on_device,
        mesh=finer,
        in_specs=(P(DP_FEAT, None, None), P(DP, None, Z), P(), P(), P(), P()),
        out_specs=(
            P(DP_FEAT, None),
            P(DP_FEAT),
            P(DP_FEAT, None),
            P(),
            P(DP_FEAT, None, None),
            P(),
        ),
        check_vma=False,
    )
```
